32 devices in a mesh: blk: 8 (over z, core), section: 4 (over y, x).
Axes of the slice: x: 2, y: 2, z: 4, core: 2. Of those that a mesh axis runs over, the one named last changes fastest.
Arguments:
- hidden: bfloat16 [4, 2048, 4096], P('section', 'blk'), parts along dimension 1, may hold values from -6 to 6
- exit_layer: int32 [4096], P('blk'), parts along dimension 0, may hold values from 1 to 2
- lengths: int32 [4096], P('blk'), parts along dimension 0, may hold values from 1 to 16, as said below
- kv_cache: bfloat16 [4, 2048, 16, 256], P('section', 'blk'), parts along dimension 1, may hold values from -256 to 256
- norm_gain: bfloat16 [4, 4096], P('section'), may hold values from 0.5 to 1.5
- w_qkv: bfloat16 [4, 4096, 1280], P('section'), may hold values from -0.0625 to 0.0625
- w_out: bfloat16 [4, 1024, 4096], P('section'), may hold values from -0.1875 to 0.1875
Outputs:
- settled: bfloat16 [4096, 8192], P('blk', 'section'), parts along dimension 0
The draws below stay inside these ranges and needn't reach their ends.
There are 8 independent parts, one for each index of `blk`. The reference program is written for one: setup_inputs(seed, part) draws one part's arguments, and reference() takes and returns one part's arrays. A program takes and returns all parts, laid end to end along the dimension named above; an argument that names none is the same for every part. Nothing has to cross between parts.
Inputs may be any that keep to these rules, and one draw needn't show every extreme that they name: `lengths`: some token has length 16.
All inputs are finite; a program needn't handle non-finite values.
Results may differ from the reference program's by a relative error of at most 0.03.
Values may be sent and summed in bfloat16 or wider, within the bound.
A program may use at most 64 MiB of HBM per device.

```python
import jax
import jax.numpy as jnp
from jax import lax

D = 8192
HD = 128
QH = 8
BLOCK = 64
MICRO = 8
CTX = 16
SHARDS = 2
LAYERS = 2
TOKENS = 512


def draw_exit_layer(key, part):
    count_key = jax.random.fold_in(key, 11)
    order_key = jax.random.fold_in(key, 13)
    depth_key = jax.random.fold_in(key, 14)
    counts = jax.random.randint(count_key, (MICRO,), BLOCK // 4, BLOCK // 2 + 1)
    scores = jax.random.randint(order_key, (MICRO, BLOCK), 0, 1 << 20) * BLOCK + jnp.arange(BLOCK)[None, :]
    ranking = jnp.argsort(jnp.argsort(scores, axis=1), axis=1)
    deeper = ranking < counts[:, None]
    depth = jax.random.randint(depth_key, (MICRO, BLOCK), 2, LAYERS + 1)
    return jnp.where(deeper, depth, 1).reshape(-1).astype(jnp.int32)


def draw_lengths(key, part):
    length_key = jax.random.fold_in(key, 21)
    forced_key = jax.random.fold_in(key, 22)
    drawn = jax.random.randint(length_key, (TOKENS,), 1, CTX + 1)
    forced = jax.random.randint(forced_key, (), 0, TOKENS)
    return jnp.where(jnp.arange(TOKENS) == forced, CTX, drawn).astype(jnp.int32)


def draw_kv_cache(key, part):
    keys_key = jax.random.fold_in(key, 31)
    values_key = jax.random.fold_in(key, 32)
    shape = (SHARDS * LAYERS, TOKENS // SHARDS, CTX, HD)
    keys = jax.random.truncated_normal(keys_key, -4.0, 4.0, shape, jnp.float32)
    values = jax.random.truncated_normal(values_key, -4.0, 4.0, shape, jnp.float32)
    return jnp.concatenate([keys, values], axis=-1).astype(jnp.bfloat16)


def steps_of(key, dims, cuts, low, largest):
    def one(dim, shards_of):
        draws = jax.random.uniform(jax.random.fold_in(jax.random.fold_in(key, 6), dim), (shards_of,), jnp.float32, low / len(cuts), largest / len(cuts))
        return jnp.repeat(jnp.exp(draws), dims[dim] // shards_of).reshape((-1,) + (1,) * (len(dims) - dim - 1))

    loudness = one(*cuts[0])
    for cut in cuts[1:]:
        loudness = loudness * one(*cut)
    return loudness


def centred(stream_key, extent, spread, limit, shards=(), held_as=jnp.bfloat16):
    values = spread * jax.random.normal(stream_key, extent, jnp.float32)
    if shards:
        values = values * steps_of(stream_key, extent, shards, -0.22, 0.18)
    return jnp.clip(values, -limit, limit).astype(held_as)


def setup_inputs(seed: int = 0, part: int = 0) -> dict:
    arg_keys = jax.random.split(jax.random.key(seed), 8)
    own_keys = jax.random.split(jax.random.fold_in(arg_keys[7], part), 8)
    hidden = centred(own_keys[0], (SHARDS * LAYERS, TOKENS // LAYERS, D // SHARDS), 1.0, 6.0, ((0, 4),))
    exit_layer = draw_exit_layer(jax.random.fold_in(jax.random.fold_in(arg_keys[7], part), 71), part)
    lengths = draw_lengths(jax.random.fold_in(jax.random.fold_in(arg_keys[7], part), 71), part)
    kv_cache = draw_kv_cache(jax.random.fold_in(jax.random.fold_in(arg_keys[7], part), 71), part)
    norm_gain = jnp.clip(1.0 + 0.1 * jax.random.normal(arg_keys[4], (SHARDS * LAYERS, D // SHARDS), jnp.float32), 0.5, 1.5).astype(jnp.bfloat16)
    w_qkv = centred(arg_keys[5], (SHARDS * LAYERS, D // SHARDS, (QH + 2) * HD), D ** -0.5, 0.0625, ((0, 4),))
    w_out = centred(arg_keys[6], (SHARDS * LAYERS, QH * HD, D // SHARDS), (QH * HD) ** -0.5, 0.1875, ((0, 4),))
    return dict(hidden=hidden, exit_layer=exit_layer, lengths=lengths, kv_cache=kv_cache, norm_gain=norm_gain, w_qkv=w_qkv, w_out=w_out)


EPSILON = 1e-05
NEGATIVE = -1e+30

def attend(state, active, len_rows, cache_rows, gain_row, proj_weight, out_weight):
    query_width = out_weight.shape[0]
    head_size = (proj_weight.shape[1] - query_width) // 2
    heads = query_width // head_size
    rows = state.shape[0]
    context = cache_rows.shape[1]
    widened = state.astype(jnp.float32)
    scaled = (widened * gain_row.astype(jnp.float32)).astype(jnp.bfloat16)
    mean_square = lax.optimization_barrier(jnp.mean(widened * widened, axis=-1))
    projected = jnp.dot(scaled, proj_weight, preferred_element_type=jnp.float32) * lax.rsqrt(mean_square + EPSILON)[:, None]
    query = (projected[:, :query_width] * (1.0 / jnp.sqrt(jnp.float32(head_size)))).astype(jnp.bfloat16)
    query = query.reshape(rows, heads, head_size).astype(jnp.float32)
    key_new = projected[:, query_width:query_width + head_size].astype(jnp.bfloat16).astype(jnp.float32)
    value_new = projected[:, query_width + head_size:].astype(jnp.bfloat16).astype(jnp.float32)
    keys = cache_rows[:, :, :head_size].astype(jnp.float32)
    values = cache_rows[:, :, head_size:].astype(jnp.float32)
    scores = jnp.einsum('rhd,rcd->rhc', query, keys)
    own = jnp.einsum('rhd,rd->rh', query, key_new)
    positions = jnp.arange(context, dtype=jnp.int32)
    usable = (positions[None, :] < len_rows[:, None])[:, None, :]
    scores = jnp.where(usable, scores, NEGATIVE)
    row_top = jnp.maximum(lax.optimization_barrier(jnp.max(scores, axis=-1)), own)
    raw = jnp.where(usable, jnp.exp(scores - row_top[:, :, None]), jnp.float32(0.0))
    raw_own = jnp.exp(own - row_top)
    total = lax.optimization_barrier(jnp.sum(raw, axis=-1)) + raw_own
    weights = (raw / total[:, :, None]).astype(jnp.bfloat16).astype(jnp.float32)
    own_weight = (raw_own / total).astype(jnp.bfloat16).astype(jnp.float32)
    attended = jnp.einsum('rhc,rcd->rhd', weights, values) + own_weight[:, :, None] * value_new[:, None, :]
    attended = attended.astype(jnp.bfloat16).reshape(rows, query_width)
    branch_out = jnp.dot(attended, out_weight, preferred_element_type=jnp.float32)
    updated = (widened + branch_out).astype(jnp.bfloat16)
    return jnp.where(active[:, None], updated, state)

def reference(hidden, exit_layer, lengths, kv_cache, norm_gain, w_qkv, w_out):
    group = BLOCK // SHARDS
    span = D // (SHARDS * LAYERS)
    columns = w_qkv.shape[2]
    query_width = w_out.shape[1]
    width = kv_cache.shape[3]
    rounds = MICRO // LAYERS
    gains = norm_gain.reshape(LAYERS, SHARDS, LAYERS, span).transpose(0, 2, 1, 3).reshape(LAYERS, D)
    projections = w_qkv.reshape(LAYERS, SHARDS, LAYERS, span, columns).transpose(0, 2, 1, 3, 4).reshape(LAYERS, D, columns)
    outputs = w_out.reshape(LAYERS, SHARDS, query_width, LAYERS, span).transpose(0, 2, 3, 1, 4).reshape(LAYERS, query_width, D)
    cache = kv_cache.reshape(LAYERS, SHARDS, MICRO, group, CTX, width).transpose(0, 2, 1, 3, 4, 5).reshape(LAYERS, MICRO * BLOCK, CTX, width)
    arranged = hidden.reshape(LAYERS, SHARDS, rounds, BLOCK, LAYERS, span).transpose(2, 0, 3, 4, 1, 5).reshape(rounds, LAYERS, BLOCK, D)
    arranged = jnp.stack([arranged[:, (LAYERS - place) % LAYERS] for place in range(LAYERS)], axis=1)
    state = arranged.reshape(MICRO * BLOCK, D)
    for layer in range(LAYERS):
        state = attend(state, exit_layer > layer, lengths, cache[layer], gains[layer], projections[layer], outputs[layer])
    return state
```

```python
import functools
import math

import jax
import jax.numpy as jnp
from jax import lax
from jax.experimental import pallas as pl
from jax.experimental.pallas import tpu as pltpu
from jax.sharding import PartitionSpec as P

BLOCK = 64
MICRO = 8


EPSILON = 1e-05
NEGATIVE = -1e30


def partner(value, axis, distance):
    return lax.ppermute(value, axis, [(i, i ^ 1 << distance) for i in range(lax.axis_size(axis))])


def shifted(value, axis, steps):
    count = lax.axis_size(axis)
    pairs = [(source, (source + steps) % count) for source in range(count)]
    return lax.ppermute(value, axis, pairs)


def body(hidden, exit_layer, lengths, kv_cache, norm_gain, w_qkv, w_out):
    devices = lax.axis_size("section")
    index = lax.axis_index("section")
    shards = max(2, devices // 4)
    cycle_size = devices // shards
    segment_bits = cycle_size.bit_length() - 1
    shard_bits = shards.bit_length() - 1
    segment_index = index // shards
    shard_index = index % shards
    own_blocks = hidden[0]
    gain_row = norm_gain[0].astype(jnp.float32)
    proj_weight = w_qkv[0]
    out_weight = w_out[0]
    cache_all = kv_cache[0]
    query_width = out_weight.shape[0]
    head_size = (proj_weight.shape[1] - query_width) // 2
    heads = query_width // head_size
    quarter = proj_weight.shape[0]
    total_width = quarter * shards
    group_rows = BLOCK // shards
    rounds = MICRO // cycle_size
    context = cache_all.shape[1]
    positions = jnp.arange(context, dtype=jnp.int32)
    blank_block = jnp.zeros((BLOCK, quarter), jnp.bfloat16)

    def advance(carry, microstep):
        incoming, arriving, records = carry
        micro_index = microstep - segment_index
        in_range = (micro_index >= 0) & (micro_index < MICRO)
        slot = jnp.clip(micro_index, 0, MICRO - 1)
        on_turn = microstep % cycle_size == 0
        local_slot = jnp.minimum(microstep // cycle_size, rounds - 1)
        own_block = lax.dynamic_slice_in_dim(own_blocks, local_slot * BLOCK, BLOCK, 0)
        exit_rows = lax.dynamic_slice_in_dim(exit_layer, slot * BLOCK, BLOCK)
        own_lengths = lax.dynamic_slice_in_dim(
            lengths, slot * BLOCK + shard_index * group_rows, group_rows
        )
        own_cache = lax.dynamic_slice_in_dim(cache_all, slot * group_rows, group_rows, 0)
        first_input = jnp.where(on_turn, own_block, arriving)
        entering = jnp.where(segment_index == 0, first_input, incoming)
        active = exit_rows > segment_index
        gate = in_range & (jnp.sum(active.astype(jnp.int32)) > 0)

        def local_partials():
            widened = entering.astype(jnp.float32)
            scaled = (widened * gain_row).astype(jnp.bfloat16)
            return (
                jnp.dot(scaled, proj_weight, preferred_element_type=jnp.float32),
                jnp.sum(widened * widened, axis=1),
            )

        def no_partials():
            return (
                jnp.zeros((BLOCK, proj_weight.shape[1]), jnp.float32),
                jnp.zeros((BLOCK,), jnp.float32),
            )

        partial_proj, partial_squares = lax.cond(gate, local_partials, no_partials)
        kept = (partial_proj, partial_squares)
        for level in range(shard_bits):
            bit = shard_bits - 1 - level
            upper = index >> bit & 1
            halves = tuple(
                (piece.reshape((2, piece.shape[0] // 2) + piece.shape[1:]) for piece in kept)
            )
            keep = tuple((jnp.where(upper == 1, half[1], half[0]) for half in halves))
            send = tuple((jnp.where(upper == 1, half[0], half[1]) for half in halves))
            received = partner(send, "section", bit)
            kept = tuple((first + second for first, second in zip(keep, received)))
        own_proj, own_squares = kept

        def local_attention():
            fitted = own_proj * lax.rsqrt(own_squares / total_width + EPSILON)[:, None]
            query = (fitted[:, :query_width] * (1.0 / math.sqrt(head_size))).astype(jnp.bfloat16)
            query = query.reshape(group_rows, heads, head_size)
            key_new = fitted[:, query_width : query_width + head_size].astype(jnp.bfloat16)
            value_new = fitted[:, query_width + head_size :].astype(jnp.bfloat16)
            scores = jnp.einsum(
                "rhd,rcd->rhc",
                query,
                own_cache[:, :, :head_size],
                preferred_element_type=jnp.float32,
            )
            own = jnp.einsum("rhd,rd->rh", query, key_new, preferred_element_type=jnp.float32)
            usable = (positions[None, :] < own_lengths[:, None])[:, None, :]
            scores = jnp.where(usable, scores, NEGATIVE)
            row_top = jnp.maximum(jnp.max(scores, axis=-1), own)
            raw = jnp.where(usable, jnp.exp(scores - row_top[:, :, None]), jnp.float32(0.0))
            raw_own = jnp.exp(own - row_top)
            total = jnp.sum(raw, axis=-1) + raw_own
            weights = (raw / total[:, :, None]).astype(jnp.bfloat16)
            own_weight = (raw_own / total).astype(jnp.bfloat16)
            attended = jnp.einsum(
                "rhc,rcd->rhd",
                weights,
                own_cache[:, :, head_size:],
                preferred_element_type=jnp.float32,
            )
            attended = (
                attended
                + own_weight.astype(jnp.float32)[:, :, None]
                * value_new.astype(jnp.float32)[:, None, :]
            )
            return attended.astype(jnp.bfloat16).reshape(group_rows, query_width)

        def no_attention():
            return jnp.zeros((group_rows, query_width), jnp.bfloat16)

        collected = lax.cond(gate, local_attention, no_attention)
        for level in range(shard_bits):
            bit = level
            other = partner(collected, "section", bit)
            upper = index >> bit & 1
            collected = jnp.where(
                upper == 1,
                jnp.concatenate([other, collected], 0),
                jnp.concatenate([collected, other], 0),
            )

        def local_update():
            branch_out = jnp.dot(collected, out_weight, preferred_element_type=jnp.float32)
            updated = (entering.astype(jnp.float32) + branch_out).astype(jnp.bfloat16)
            return jnp.where(active[:, None], updated, entering)

        def keep_state():
            return entering

        outgoing = lax.cond(gate, local_update, keep_state)
        leaving = in_range & (exit_rows == segment_index + 1)
        previous = lax.dynamic_slice_in_dim(records, slot * BLOCK, BLOCK, 0)
        records = lax.dynamic_update_slice_in_dim(
            records, jnp.where(leaving[:, None], outgoing, previous), slot * BLOCK, 0
        )
        relayed = jnp.where(on_turn & (segment_index > 0), own_block, arriving)
        incoming, arriving = shifted((outgoing, relayed), "section", shards)
        return ((incoming, arriving, records), None)

    start = (blank_block, blank_block, jnp.zeros((MICRO * BLOCK, quarter), jnp.bfloat16))
    carry, _ = lax.scan(advance, start, jnp.arange(MICRO + cycle_size - 1, dtype=jnp.int32))
    kept = carry[2]
    for level in range(segment_bits):
        bit = shard_bits + segment_bits - 1 - level
        upper = index >> bit & 1
        halves = kept.reshape(kept.shape[0], 2, kept.shape[1] // 2)
        keep = jnp.where(upper == 1, halves[:, 1], halves[:, 0])
        send = jnp.where(upper == 1, halves[:, 0], halves[:, 1])
        received = partner(send, "section", bit)
        kept = (keep.astype(jnp.float32) + received.astype(jnp.float32)).astype(jnp.bfloat16)
    return kept


MESH = pl.DeviceIdType.MESH


def cycle_kernel(
    sizes,
    hidden,
    tokens,
    cache_hbm,
    gain,
    wq_hbm,
    wo_hbm,
    out,
    wq,
    wo,
    cache,
    stage,
    ready,
    scaled,
    partial,
    squares,
    psend,
    precv,
    att,
    load_sem,
    own_sem,
    st_send,
    st_recv,
    p_send,
    p_recv,
    a_send,
    a_recv,
    out_send,
    out_recv,
    keep_sem,
):
    shards, head_size, heads = sizes
    index = lax.axis_index("section")
    seg = index // shards
    shard = index % shards
    across = seg * shards + (1 - shard)
    along = (1 - seg) * shards + shard
    width = stage.shape[2]
    columns = wq.shape[1]
    query_width = heads * head_size
    half = MICRO // 2
    rows = BLOCK // shards
    span = out.shape[1]
    context = cache.shape[1]
    own_rows = pl.ds(pl.multiple_of(shard * rows, rows), rows)
    other_rows = pl.ds(pl.multiple_of((1 - shard) * rows, rows), rows)

    barrier = pltpu.get_barrier_semaphore()
    for peer in (across, along):
        pl.semaphore_signal(barrier, inc=1, device_id={"section": peer}, device_id_type=MESH)

    def own_copy(i):
        return pltpu.make_async_copy(
            hidden.at[pl.ds(i * BLOCK, BLOCK)], stage.at[i], own_sem.at[i]
        )

    load_wq = pltpu.make_async_copy(wq_hbm, wq, load_sem.at[0])
    load_cache = pltpu.make_async_copy(cache_hbm, cache, load_sem.at[1])
    load_wo = pltpu.make_async_copy(wo_hbm, wo, load_sem.at[2])

    @pl.when(seg == 0)
    def _():
        own_copy(0).start()

    load_wq.start()
    load_cache.start()
    load_wo.start()

    def place(i):
        return jnp.where(i < half, 2 * i, 2 * (i - half) + 1)

    def hidden_copy(i):
        return pltpu.make_async_remote_copy(
            src_ref=hidden.at[pl.ds(i * BLOCK, BLOCK)],
            dst_ref=stage.at[half + i],
            send_sem=st_send.at[half + i],
            recv_sem=st_recv.at[half + i],
            device_id={"section": along},
            device_id_type=MESH,
        )

    def state_copy(i):
        return pltpu.make_async_remote_copy(
            src_ref=ready.at[i],
            dst_ref=stage.at[i],
            send_sem=st_send.at[i],
            recv_sem=st_recv.at[i],
            device_id={"section": along},
            device_id_type=MESH,
        )

    def partial_copy(i):
        return pltpu.make_async_remote_copy(
            src_ref=psend.at[i],
            dst_ref=precv.at[i],
            send_sem=p_send.at[i],
            recv_sem=p_recv.at[i],
            device_id={"section": across},
            device_id_type=MESH,
        )

    def attended_copy(i, sent_rows):
        return pltpu.make_async_remote_copy(
            src_ref=att.at[i, sent_rows],
            dst_ref=att.at[i, sent_rows],
            send_sem=a_send.at[i],
            recv_sem=a_recv.at[i],
            device_id={"section": across},
            device_id_type=MESH,
        )

    def out_rows(i):
        return pl.ds(pl.multiple_of(place(i) * BLOCK, BLOCK), BLOCK)

    def settled_copy(i):
        return pltpu.make_async_remote_copy(
            src_ref=ready.at[i, :, pl.ds(0, span)],
            dst_ref=out.at[out_rows(i)],
            send_sem=out_send.at[i],
            recv_sem=out_recv.at[i],
            device_id={"section": along},
            device_id_type=MESH,
        )

    def kept_copy(i):
        return pltpu.make_async_copy(
            ready.at[i, :, pl.ds(span, span)], out.at[out_rows(i)], keep_sem.at[i]
        )

    pl.semaphore_wait(barrier, 2)

    @pl.when(seg == 1)
    def _():
        for i in range(half):
            hidden_copy(i).start()

    @pl.when(seg == 0)
    def _():
        for i in range(1, half):
            own_copy(i).start()

    def project(i):
        local = (seg == 0) & (i < half)

        @pl.when(local)
        def _():
            own_copy(i).wait()

        @pl.when(jnp.logical_not(local))
        def _():
            state_copy(i).wait_recv()

        @pl.when(i == 0)
        def _():
            load_wq.wait()

        chunk = min(width, 512)
        total = jnp.zeros((BLOCK, 1), jnp.float32)
        for start in range(0, width, chunk):
            cols = pl.ds(start, chunk)
            piece = stage[i, :, cols].astype(jnp.float32)
            total = total + jnp.sum(piece * piece, axis=1, keepdims=True)
            scaled[:, cols] = (piece * gain[:, cols].astype(jnp.float32)).astype(jnp.bfloat16)
        squares[...] = jnp.broadcast_to(total, squares.shape)
        step = 512
        for start in range(0, columns, step):
            cols = pl.ds(start, min(step, columns - start))
            partial[:, cols] = jnp.dot(
                scaled[...], wq[:, cols], preferred_element_type=jnp.float32
            )
        psend[i, :, pl.ds(0, columns)] = partial[other_rows, :].astype(jnp.bfloat16)
        theirs = squares[other_rows, :]
        coarse = theirs.astype(jnp.bfloat16)
        fine = (theirs - coarse.astype(jnp.float32)).astype(jnp.bfloat16)
        psend[i, :, pl.ds(columns, 128)] = coarse
        psend[i, :, pl.ds(columns + 128, 128)] = fine
        partial_copy(i).start()

    def attend_rows(i):
        @pl.when(i == 0)
        def _():
            load_cache.wait()

        partial_copy(i).wait_recv()
        coarse = precv[i, :, pl.ds(columns, 128)].astype(jnp.float32)
        fine = precv[i, :, pl.ds(columns + 128, 128)].astype(jnp.float32)
        total_squares = squares[own_rows, :] + coarse + fine
        factor = lax.rsqrt(total_squares / (width * shards) + EPSILON)[:, :1]
        fitted = (
            partial[own_rows, :] + precv[i, :, pl.ds(0, columns)].astype(jnp.float32)
        ) * factor
        scale = 1.0 / math.sqrt(head_size)
        query = jnp.concatenate(
            [fitted[:, h * head_size : (h + 1) * head_size] for h in range(heads)], axis=0
        )
        query = (query * scale).astype(jnp.bfloat16)
        key_new = fitted[:, query_width : query_width + head_size].astype(jnp.bfloat16)
        value_new = fitted[:, query_width + head_size :].astype(jnp.bfloat16)
        key_new = jnp.concatenate([key_new.astype(jnp.float32)] * heads, axis=0)
        value_new = jnp.concatenate([value_new.astype(jnp.float32)] * heads, axis=0)
        start = pl.multiple_of(place(i) * rows, rows)
        held = cache[pl.ds(start, rows)].reshape(rows * context, 2 * head_size)
        scores = lax.dot_general(
            query,
            held[:, :head_size],
            (((1,), (1,)), ((), ())),
            preferred_element_type=jnp.float32,
        )
        own = jnp.sum(query.astype(jnp.float32) * key_new, axis=1, keepdims=True)
        limits = tokens[pl.ds(pl.multiple_of(place(i) * BLOCK + shard * rows, rows), rows), :][:, 1:2]
        row = lax.broadcasted_iota(jnp.int32, (rows, 1), 0) * context
        low = jnp.concatenate([row] * heads, axis=0)
        high = jnp.concatenate([row + limits] * heads, axis=0)
        column = lax.broadcasted_iota(jnp.int32, scores.shape, 1)
        usable = (column >= low) & (column < high)
        scores = jnp.where(usable, scores, NEGATIVE)
        row_top = jnp.maximum(jnp.max(scores, axis=1, keepdims=True), own)
        raw = jnp.where(usable, jnp.exp(scores - row_top), 0.0)
        raw_own = jnp.exp(own - row_top)
        total = jnp.sum(raw, axis=1, keepdims=True) + raw_own
        weights = (raw / total).astype(jnp.bfloat16)
        own_weight = (raw_own / total).astype(jnp.bfloat16).astype(jnp.float32)
        attended = jnp.dot(
            weights, held[:, head_size:], preferred_element_type=jnp.float32
        )
        attended = (attended + own_weight * value_new).astype(jnp.bfloat16)
        att[i, own_rows, :] = jnp.concatenate(
            [attended[h * rows : (h + 1) * rows] for h in range(heads)], axis=1
        )
        attended_copy(i, own_rows).start()

    def update(i):
        @pl.when(i == 0)
        def _():
            load_wo.wait()

        attended_copy(i, other_rows).wait_recv()
        depth = tokens[pl.ds(pl.multiple_of(place(i) * BLOCK, BLOCK), BLOCK), :][:, 0:1]
        active = depth > seg
        step = min(width, 512)
        for start in range(0, width, step):
            cols = pl.ds(start, step)
            branch = jnp.dot(att[i], wo[:, cols], preferred_element_type=jnp.float32)
            before = stage[i, :, cols].astype(jnp.float32)
            ready[i, :, cols] = jnp.where(active, before + branch, before).astype(jnp.bfloat16)

        @pl.when(seg == 0)
        def _():
            state_copy(i).start()

        @pl.when(seg == 1)
        def _():
            settled_copy(i).start()
            kept_copy(i).start()

    def step(i, carry):
        @pl.when(i < MICRO)
        def _():
            project(i)

        @pl.when(i > 0)
        def _():
            update(i - 1)

        @pl.when(i < MICRO)
        def _():
            attend_rows(i)

        return carry

    lax.fori_loop(0, MICRO + 1, step, 0)

    def drain(i, carry):
        partial_copy(i).wait_send()
        attended_copy(i, own_rows).wait_send()

        @pl.when(seg == 0)
        def _():
            state_copy(i).wait_send()
            settled_copy(i).wait_recv()

        @pl.when(seg == 1)
        def _():
            settled_copy(i).wait_send()
            kept_copy(i).wait()

        return carry

    lax.fori_loop(0, MICRO, drain, 0)

    @pl.when(seg == 1)
    def _():
        for i in range(half):
            hidden_copy(i).wait_send()


def cycle_of_two(hidden, exit_layer, lengths, kv_cache, norm_gain, w_qkv, w_out):
    shards = 2
    width = w_qkv.shape[1]
    columns = w_qkv.shape[2]
    query_width = w_out.shape[1]
    head_size = (columns - query_width) // 2
    heads = query_width // head_size
    rows = BLOCK // shards
    tokens = jnp.stack([exit_layer, lengths], axis=1)
    any_space = pl.BlockSpec(memory_space=pl.ANY)
    vmem = pl.BlockSpec(memory_space=pltpu.VMEM)
    dma = pltpu.SemaphoreType.DMA((MICRO,))
    bf16 = jnp.bfloat16
    return pl.pallas_call(
        functools.partial(cycle_kernel, (shards, head_size, heads)),
        out_shape=jax.ShapeDtypeStruct((MICRO * BLOCK, width // 2), bf16),
        in_specs=[any_space, vmem, any_space, vmem, any_space, any_space],
        out_specs=any_space,
        scratch_shapes=[
            pltpu.VMEM(w_qkv.shape[1:], bf16),
            pltpu.VMEM(w_out.shape[1:], bf16),
            pltpu.VMEM(kv_cache.shape[1:], bf16),
            pltpu.VMEM((MICRO, BLOCK, width), bf16),
            pltpu.VMEM((MICRO, BLOCK, width), bf16),
            pltpu.VMEM((BLOCK, width), bf16),
            pltpu.VMEM((BLOCK, columns), jnp.float32),
            pltpu.VMEM((BLOCK, 128), jnp.float32),
            pltpu.VMEM((MICRO, rows, columns + 256), bf16),
            pltpu.VMEM((MICRO, rows, columns + 256), bf16),
            pltpu.VMEM((MICRO, BLOCK, query_width), bf16),
            pltpu.SemaphoreType.DMA((3,)),
        ]
        + [dma] * 10,
        compiler_params=pltpu.CompilerParams(
            collective_id=0, has_side_effects=True, vmem_limit_bytes=60 << 20
        ),
        name="cycle",
    )(hidden[0], tokens, kv_cache[0], norm_gain, w_qkv[0], w_out[0])


def chosen(devices, *arguments):
    shards = max(2, devices // 4)
    if shards == 2 and devices // shards == 2:
        return cycle_of_two(*arguments)
    return body(*arguments)


def solution(mesh):
    return jax.shard_map(
        functools.partial(chosen, mesh.shape["section"]),
        mesh=mesh,
        in_specs=(
            P("section", "blk", None),
            P("blk"),
            P("blk"),
            P("section", "blk", None, None),
            P("section", None),
            P("section", None, None),
            P("section", None, None),
        ),
        out_specs=P("blk", "section"),
        check_vma=False,
    )
```

```python
import functools
import math

import jax
import jax.numpy as jnp
from jax import lax
from jax.experimental import pallas as pl
from jax.experimental.pallas import tpu as pltpu
from jax.sharding import PartitionSpec as P

BLOCK = 64
MICRO = 8


EPSILON = 1e-05
NEGATIVE = -1e30


def partner(value, axis, distance):
    return lax.ppermute(value, axis, [(i, i ^ 1 << distance) for i in range(lax.axis_size(axis))])


def shifted(value, axis, steps):
    count = lax.axis_size(axis)
    pairs = [(source, (source + steps) % count) for source in range(count)]
    return lax.ppermute(value, axis, pairs)


def body(hidden, exit_layer, lengths, kv_cache, norm_gain, w_qkv, w_out):
    devices = lax.axis_size("section")
    index = lax.axis_index("section")
    shards = max(2, devices // 4)
    cycle_size = devices // shards
    segment_bits = cycle_size.bit_length() - 1
    shard_bits = shards.bit_length() - 1
    segment_index = index // shards
    shard_index = index % shards
    own_blocks = hidden[0]
    gain_row = norm_gain[0].astype(jnp.float32)
    proj_weight = w_qkv[0]
    out_weight = w_out[0]
    cache_all = kv_cache[0]
    query_width = out_weight.shape[0]
    head_size = (proj_weight.shape[1] - query_width) // 2
    heads = query_width // head_size
    quarter = proj_weight.shape[0]
    total_width = quarter * shards
    group_rows = BLOCK // shards
    rounds = MICRO // cycle_size
    context = cache_all.shape[1]
    positions = jnp.arange(context, dtype=jnp.int32)
    blank_block = jnp.zeros((BLOCK, quarter), jnp.bfloat16)

    def advance(carry, microstep):
        incoming, arriving, records = carry
        micro_index = microstep - segment_index
        in_range = (micro_index >= 0) & (micro_index < MICRO)
        slot = jnp.clip(micro_index, 0, MICRO - 1)
        on_turn = microstep % cycle_size == 0
        local_slot = jnp.minimum(microstep // cycle_size, rounds - 1)
        own_block = lax.dynamic_slice_in_dim(own_blocks, local_slot * BLOCK, BLOCK, 0)
        exit_rows = lax.dynamic_slice_in_dim(exit_layer, slot * BLOCK, BLOCK)
        own_lengths = lax.dynamic_slice_in_dim(
            lengths, slot * BLOCK + shard_index * group_rows, group_rows
        )
        own_cache = lax.dynamic_slice_in_dim(cache_all, slot * group_rows, group_rows, 0)
        first_input = jnp.where(on_turn, own_block, arriving)
        entering = jnp.where(segment_index == 0, first_input, incoming)
        active = exit_rows > segment_index
        gate = in_range & (jnp.sum(active.astype(jnp.int32)) > 0)

        def local_partials():
            widened = entering.astype(jnp.float32)
            scaled = (widened * gain_row).astype(jnp.bfloat16)
            return (
                jnp.dot(scaled, proj_weight, preferred_element_type=jnp.float32),
                jnp.sum(widened * widened, axis=1),
            )

        def no_partials():
            return (
                jnp.zeros((BLOCK, proj_weight.shape[1]), jnp.float32),
                jnp.zeros((BLOCK,), jnp.float32),
            )

        partial_proj, partial_squares = lax.cond(gate, local_partials, no_partials)
        kept = (partial_proj, partial_squares)
        for level in range(shard_bits):
            bit = shard_bits - 1 - level
            upper = index >> bit & 1
            halves = tuple(
                (piece.reshape((2, piece.shape[0] // 2) + piece.shape[1:]) for piece in kept)
            )
            keep = tuple((jnp.where(upper == 1, half[1], half[0]) for half in halves))
            send = tuple((jnp.where(upper == 1, half[0], half[1]) for half in halves))
            received = partner(send, "section", bit)
            kept = tuple((first + second for first, second in zip(keep, received)))
        own_proj, own_squares = kept

        def local_attention():
            fitted = own_proj * lax.rsqrt(own_squares / total_width + EPSILON)[:, None]
            query = (fitted[:, :query_width] * (1.0 / math.sqrt(head_size))).astype(jnp.bfloat16)
            query = query.reshape(group_rows, heads, head_size)
            key_new = fitted[:, query_width : query_width + head_size].astype(jnp.bfloat16)
            value_new = fitted[:, query_width + head_size :].astype(jnp.bfloat16)
            scores = jnp.einsum(
                "rhd,rcd->rhc",
                query,
                own_cache[:, :, :head_size],
                preferred_element_type=jnp.float32,
            )
            own = jnp.einsum("rhd,rd->rh", query, key_new, preferred_element_type=jnp.float32)
            usable = (positions[None, :] < own_lengths[:, None])[:, None, :]
            scores = jnp.where(usable, scores, NEGATIVE)
            row_top = jnp.maximum(jnp.max(scores, axis=-1), own)
            raw = jnp.where(usable, jnp.exp(scores - row_top[:, :, None]), jnp.float32(0.0))
            raw_own = jnp.exp(own - row_top)
            total = jnp.sum(raw, axis=-1) + raw_own
            weights = (raw / total[:, :, None]).astype(jnp.bfloat16)
            own_weight = (raw_own / total).astype(jnp.bfloat16)
            attended = jnp.einsum(
                "rhc,rcd->rhd",
                weights,
                own_cache[:, :, head_size:],
                preferred_element_type=jnp.float32,
            )
            attended = (
                attended
                + own_weight.astype(jnp.float32)[:, :, None]
                * value_new.astype(jnp.float32)[:, None, :]
            )
            return attended.astype(jnp.bfloat16).reshape(group_rows, query_width)

        def no_attention():
            return jnp.zeros((group_rows, query_width), jnp.bfloat16)

        collected = lax.cond(gate, local_attention, no_attention)
        for level in range(shard_bits):
            bit = level
            other = partner(collected, "section", bit)
            upper = index >> bit & 1
            collected = jnp.where(
                upper == 1,
                jnp.concatenate([other, collected], 0),
                jnp.concatenate([collected, other], 0),
            )

        def local_update():
            branch_out = jnp.dot(collected, out_weight, preferred_element_type=jnp.float32)
            updated = (entering.astype(jnp.float32) + branch_out).astype(jnp.bfloat16)
            return jnp.where(active[:, None], updated, entering)

        def keep_state():
            return entering

        outgoing = lax.cond(gate, local_update, keep_state)
        leaving = in_range & (exit_rows == segment_index + 1)
        previous = lax.dynamic_slice_in_dim(records, slot * BLOCK, BLOCK, 0)
        records = lax.dynamic_update_slice_in_dim(
            records, jnp.where(leaving[:, None], outgoing, previous), slot * BLOCK, 0
        )
        relayed = jnp.where(on_turn & (segment_index > 0), own_block, arriving)
        incoming, arriving = shifted((outgoing, relayed), "section", shards)
        return ((incoming, arriving, records), None)

    start = (blank_block, blank_block, jnp.zeros((MICRO * BLOCK, quarter), jnp.bfloat16))
    carry, _ = lax.scan(advance, start, jnp.arange(MICRO + cycle_size - 1, dtype=jnp.int32))
    kept = carry[2]
    for level in range(segment_bits):
        bit = shard_bits + segment_bits - 1 - level
        upper = index >> bit & 1
        halves = kept.reshape(kept.shape[0], 2, kept.shape[1] // 2)
        keep = jnp.where(upper == 1, halves[:, 1], halves[:, 0])
        send = jnp.where(upper == 1, halves[:, 0], halves[:, 1])
        received = partner(send, "section", bit)
        kept = (keep.astype(jnp.float32) + received.astype(jnp.float32)).astype(jnp.bfloat16)
    return kept


MESH = pl.DeviceIdType.MESH


def cycle_kernel(
    sizes,
    hidden,
    tokens,
    cache_hbm,
    gain,
    wq_hbm,
    wo_hbm,
    out,
    wq,
    wo,
    cache,
    stage,
    ready,
    scaled,
    partial,
    squares,
    psend,
    precv,
    att,
    wx,
    att_in,
    load_sem,
    wy_send,
    wy_recv,
    wz_send,
    wz_recv,
    wd_send,
    wd_recv,
    own_sem,
    h_send,
    h_recv,
    lo_send,
    lo_recv,
    hi_send,
    hi_recv,
    p_send,
    p_recv,
    a_send,
    a_recv,
    out_send,
    out_recv,
    keep_sem,
):
    shards, head_size, heads = sizes
    index = lax.axis_index("section")
    seg = index // shards
    shard = index % shards
    across = seg * shards + (1 - shard)
    along = (1 - seg) * shards + shard
    width = stage.shape[2]
    columns = wq.shape[1]
    query_width = heads * head_size
    half = MICRO // 2
    rows = BLOCK // shards
    span = out.shape[1]
    context = cache.shape[1]
    own_rows = pl.ds(pl.multiple_of(shard * rows, rows), rows)
    other_rows = pl.ds(pl.multiple_of((1 - shard) * rows, rows), rows)

    place_blk = lax.axis_index("blk")
    chips = wz_send.shape[0] + 1
    chip = place_blk // 2
    core = place_blk % 2
    piece = wx.shape[0] // (2 * chips)

    def on_chip(steps):
        return (chip + steps + chips) % chips

    barrier = pltpu.get_barrier_semaphore()
    for peer in (across, along):
        pl.semaphore_signal(barrier, inc=1, device_id={"section": peer}, device_id_type=MESH)
    for steps in range(1, chips):
        pl.semaphore_signal(
            barrier,
            inc=1,
            device_id={"blk": on_chip(steps) * 2 + core},
            device_id_type=MESH,
        )
    pl.semaphore_signal(
        barrier, inc=1, device_id={"blk": chip * 2 + 1 - core}, device_id_type=MESH
    )

    def piece_rows(owner):
        return pl.ds(pl.multiple_of(owner * piece, piece), piece)

    def weight_along():
        return pltpu.make_async_remote_copy(
            src_ref=wo_hbm.at[piece_rows(place_blk), pl.ds(span, span)],
            dst_ref=wx.at[piece_rows(place_blk)],
            send_sem=wy_send.at[0],
            recv_sem=wy_recv.at[0],
            device_id={"section": along},
            device_id_type=MESH,
        )

    def weight_chips(steps, owner):
        return pltpu.make_async_remote_copy(
            src_ref=wx.at[piece_rows(owner)],
            dst_ref=wx.at[piece_rows(owner)],
            send_sem=wz_send.at[steps - 1],
            recv_sem=wz_recv.at[steps - 1],
            device_id={"blk": on_chip(steps) * 2 + core},
            device_id_type=MESH,
        )

    def weight_cores(steps, owner):
        return pltpu.make_async_remote_copy(
            src_ref=wx.at[piece_rows(owner)],
            dst_ref=wx.at[piece_rows(owner)],
            send_sem=wd_send.at[steps],
            recv_sem=wd_recv.at[steps],
            device_id={"blk": chip * 2 + 1 - core},
            device_id_type=MESH,
        )

    def own_copy(i):
        return pltpu.make_async_copy(
            hidden.at[pl.ds(i * BLOCK, BLOCK)], stage.at[i], own_sem.at[i]
        )

    def rest_copy(i):
        return pltpu.make_async_copy(
            hidden.at[pl.ds(i * BLOCK, BLOCK), pl.ds(span, span)],
            stage.at[half + i, :, pl.ds(span, span)],
            own_sem.at[i],
        )

    load_wq = pltpu.make_async_copy(wq_hbm, wq, load_sem.at[0])
    load_cache = pltpu.make_async_copy(cache_hbm, cache, load_sem.at[1])
    load_wo = pltpu.make_async_copy(wo_hbm, wo, load_sem.at[2])

    @pl.when(seg == 0)
    def _():
        own_copy(0).start()

    load_wq.start()
    load_cache.start()

    def place(i):
        return jnp.where(i < half, 2 * i, 2 * (i - half) + 1)

    def hidden_copy(i):
        return pltpu.make_async_remote_copy(
            src_ref=hidden.at[pl.ds(i * BLOCK, BLOCK)],
            dst_ref=stage.at[half + i],
            send_sem=h_send.at[i],
            recv_sem=h_recv.at[i],
            device_id={"section": along},
            device_id_type=MESH,
        )

    def low_copy(i):
        return pltpu.make_async_remote_copy(
            src_ref=ready.at[i, :, pl.ds(0, span)],
            dst_ref=stage.at[i, :, pl.ds(0, span)],
            send_sem=lo_send.at[i],
            recv_sem=lo_recv.at[i],
            device_id={"section": along},
            device_id_type=MESH,
        )

    def high_copy(i):
        return pltpu.make_async_remote_copy(
            src_ref=ready.at[i, :, pl.ds(span, span)],
            dst_ref=stage.at[i, :, pl.ds(span, span)],
            send_sem=hi_send.at[i],
            recv_sem=hi_recv.at[i],
            device_id={"section": along},
            device_id_type=MESH,
        )

    def branch_copy(i):
        return pltpu.make_async_remote_copy(
            src_ref=att.at[i],
            dst_ref=att_in.at[i - half],
            send_sem=hi_send.at[i],
            recv_sem=hi_recv.at[i],
            device_id={"section": along},
            device_id_type=MESH,
        )

    def partial_copy(i):
        return pltpu.make_async_remote_copy(
            src_ref=psend.at[i],
            dst_ref=precv.at[i],
            send_sem=p_send.at[i],
            recv_sem=p_recv.at[i],
            device_id={"section": across},
            device_id_type=MESH,
        )

    def attended_copy(i, sent_rows):
        return pltpu.make_async_remote_copy(
            src_ref=att.at[i, sent_rows],
            dst_ref=att.at[i, sent_rows],
            send_sem=a_send.at[i],
            recv_sem=a_recv.at[i],
            device_id={"section": across},
            device_id_type=MESH,
        )

    def out_rows(i):
        return pl.ds(pl.multiple_of(place(i) * BLOCK, BLOCK), BLOCK)

    def settled_copy(i):
        return pltpu.make_async_remote_copy(
            src_ref=ready.at[i, :, pl.ds(0, span)],
            dst_ref=out.at[out_rows(i)],
            send_sem=out_send.at[i],
            recv_sem=out_recv.at[i],
            device_id={"section": along},
            device_id_type=MESH,
        )

    def kept_copy(i):
        return pltpu.make_async_copy(
            ready.at[i, :, pl.ds(span, span)], out.at[out_rows(i)], keep_sem.at[i]
        )

    pl.semaphore_wait(barrier, chips + 2)

    @pl.when(seg == 0)
    def _():
        weight_along().start()
        for i in range(1, half):
            own_copy(i).start()

    @pl.when(seg == 1)
    def _():
        for i in range(half):
            hidden_copy(i).start()
        for i in range(half):
            rest_copy(i).start()
        weight_along().wait_recv()
        for steps in range(1, chips):
            weight_chips(steps, place_blk).start()
        weight_cores(0, place_blk).start()

    def project(i):
        local = (seg == 0) & (i < half)

        @pl.when(local)
        def _():
            own_copy(i).wait()

        @pl.when((seg == 0) & (i >= half))
        def _():
            hidden_copy(i - half).wait_recv()

        @pl.when((seg == 1) & (i == half - 1))
        def _():
            for steps in range(1, chips):
                owner = on_chip(-steps) * 2 + core
                weight_chips(steps, owner).wait_recv()
                weight_cores(steps, owner).start()

        @pl.when((seg == 1) & (i < half))
        def _():
            high_copy(i).wait_recv()

        @pl.when((seg == 1) & (i == half))
        def _():
            for steps in range(chips):
                weight_cores(steps, on_chip(-steps) * 2 + 1 - core).wait_recv()

        @pl.when((seg == 1) & (i >= half))
        def _():
            rest_copy(i - half).wait()
            branch_copy(i).wait_recv()
            depth = tokens[pl.ds(pl.multiple_of(place(i) * BLOCK, BLOCK), BLOCK), :][:, 0:1]
            size = min(span, 512)
            for start in range(0, span, size):
                branch = jnp.dot(
                    att_in[i - half],
                    wx[:, pl.ds(start, size)],
                    preferred_element_type=jnp.float32,
                )
                cols = pl.ds(span + start, size)
                before = stage[i, :, cols].astype(jnp.float32)
                stage[i, :, cols] = jnp.where(depth > 0, before + branch, before).astype(
                    jnp.bfloat16
                )

        @pl.when(seg == 1)
        def _():
            low_copy(i).wait_recv()

        @pl.when(i == 0)
        def _():
            load_wq.wait()
            load_wo.start()

        chunk = min(width, 512)
        total = jnp.zeros((BLOCK, 1), jnp.float32)
        for start in range(0, width, chunk):
            cols = pl.ds(start, chunk)
            piece = stage[i, :, cols].astype(jnp.float32)
            total = total + jnp.sum(piece * piece, axis=1, keepdims=True)
            scaled[:, cols] = (piece * gain[:, cols].astype(jnp.float32)).astype(jnp.bfloat16)
        squares[...] = jnp.broadcast_to(total, squares.shape)
        step = 512
        for start in range(0, columns, step):
            cols = pl.ds(start, min(step, columns - start))
            partial[:, cols] = jnp.dot(
                scaled[...], wq[:, cols], preferred_element_type=jnp.float32
            )
        psend[i, :, pl.ds(0, columns)] = partial[other_rows, :].astype(jnp.bfloat16)
        theirs = squares[other_rows, :]
        coarse = theirs.astype(jnp.bfloat16)
        fine = (theirs - coarse.astype(jnp.float32)).astype(jnp.bfloat16)
        psend[i, :, pl.ds(columns, 128)] = coarse
        psend[i, :, pl.ds(columns + 128, 128)] = fine
        partial_copy(i).start()

    def attend_rows(i):
        @pl.when(i == 0)
        def _():
            load_cache.wait()

        partial_copy(i).wait_recv()
        coarse = precv[i, :, pl.ds(columns, 128)].astype(jnp.float32)
        fine = precv[i, :, pl.ds(columns + 128, 128)].astype(jnp.float32)
        total_squares = squares[own_rows, :] + coarse + fine
        factor = lax.rsqrt(total_squares / (width * shards) + EPSILON)[:, :1]
        fitted = (
            partial[own_rows, :] + precv[i, :, pl.ds(0, columns)].astype(jnp.float32)
        ) * factor
        scale = 1.0 / math.sqrt(head_size)
        query = jnp.concatenate(
            [fitted[:, h * head_size : (h + 1) * head_size] for h in range(heads)], axis=0
        )
        query = (query * scale).astype(jnp.bfloat16)
        key_new = fitted[:, query_width : query_width + head_size].astype(jnp.bfloat16)
        value_new = fitted[:, query_width + head_size :].astype(jnp.bfloat16)
        key_new = jnp.concatenate([key_new.astype(jnp.float32)] * heads, axis=0)
        value_new = jnp.concatenate([value_new.astype(jnp.float32)] * heads, axis=0)
        start = pl.multiple_of(place(i) * rows, rows)
        held = cache[pl.ds(start, rows)].reshape(rows * context, 2 * head_size)
        scores = lax.dot_general(
            query,
            held[:, :head_size],
            (((1,), (1,)), ((), ())),
            preferred_element_type=jnp.float32,
        )
        own = jnp.sum(query.astype(jnp.float32) * key_new, axis=1, keepdims=True)
        limits = tokens[pl.ds(pl.multiple_of(place(i) * BLOCK + shard * rows, rows), rows), :][:, 1:2]
        row = lax.broadcasted_iota(jnp.int32, (rows, 1), 0) * context
        low = jnp.concatenate([row] * heads, axis=0)
        high = jnp.concatenate([row + limits] * heads, axis=0)
        column = lax.broadcasted_iota(jnp.int32, scores.shape, 1)
        usable = (column >= low) & (column < high)
        scores = jnp.where(usable, scores, NEGATIVE)
        row_top = jnp.maximum(jnp.max(scores, axis=1, keepdims=True), own)
        raw = jnp.where(usable, jnp.exp(scores - row_top), 0.0)
        raw_own = jnp.exp(own - row_top)
        total = jnp.sum(raw, axis=1, keepdims=True) + raw_own
        weights = (raw / total).astype(jnp.bfloat16)
        own_weight = (raw_own / total).astype(jnp.bfloat16).astype(jnp.float32)
        attended = jnp.dot(
            weights, held[:, head_size:], preferred_element_type=jnp.float32
        )
        attended = (attended + own_weight * value_new).astype(jnp.bfloat16)
        att[i, own_rows, :] = jnp.concatenate(
            [attended[h * rows : (h + 1) * rows] for h in range(heads)], axis=1
        )
        attended_copy(i, own_rows).start()

    def update(i):
        @pl.when(i == 0)
        def _():
            load_wo.wait()

        attended_copy(i, other_rows).wait_recv()
        depth = tokens[pl.ds(pl.multiple_of(place(i) * BLOCK, BLOCK), BLOCK), :][:, 0:1]
        active = depth > seg
        step = min(span, 512)
        brief = (seg == 0) & (i >= half)

        def fill(first):
            for start in range(first, first + span, step):
                cols = pl.ds(start, step)
                branch = jnp.dot(att[i], wo[:, cols], preferred_element_type=jnp.float32)
                before = stage[i, :, cols].astype(jnp.float32)
                ready[i, :, cols] = jnp.where(active, before + branch, before).astype(jnp.bfloat16)

        @pl.when(brief)
        def _():
            branch_copy(i).start()

        fill(0)

        @pl.when(seg == 0)
        def _():
            low_copy(i).start()

        @pl.when(seg == 1)
        def _():
            settled_copy(i).start()

        @pl.when(jnp.logical_not(brief))
        def _():
            fill(span)

        @pl.when((seg == 0) & (i < half))
        def _():
            high_copy(i).start()

        @pl.when(seg == 1)
        def _():
            kept_copy(i).start()

    def step(i, carry):
        @pl.when(i < MICRO)
        def _():
            project(i)

        @pl.when(i > 0)
        def _():
            update(i - 1)

        @pl.when(i < MICRO)
        def _():
            attend_rows(i)

        return carry

    lax.fori_loop(0, MICRO + 1, step, 0)

    def drain(i, carry):
        partial_copy(i).wait_send()
        attended_copy(i, own_rows).wait_send()

        @pl.when(seg == 0)
        def _():
            low_copy(i).wait_send()
            settled_copy(i).wait_recv()

        @pl.when(seg == 1)
        def _():
            settled_copy(i).wait_send()
            kept_copy(i).wait()

        return carry

    lax.fori_loop(0, MICRO, drain, 0)

    @pl.when(seg == 0)
    def _():
        weight_along().wait_send()
        for i in range(half):
            high_copy(i).wait_send()
            branch_copy(half + i).wait_send()

    @pl.when(seg == 1)
    def _():
        for i in range(half):
            hidden_copy(i).wait_send()
        for steps in range(1, chips):
            weight_chips(steps, place_blk).wait_send()
        for steps in range(chips):
            weight_cores(steps, on_chip(-steps) * 2 + core).wait_send()


def cycle_of_two(chips, hidden, exit_layer, lengths, kv_cache, norm_gain, w_qkv, w_out):
    shards = 2
    width = w_qkv.shape[1]
    columns = w_qkv.shape[2]
    query_width = w_out.shape[1]
    head_size = (columns - query_width) // 2
    heads = query_width // head_size
    rows = BLOCK // shards
    tokens = jnp.stack([exit_layer, lengths], axis=1)
    any_space = pl.BlockSpec(memory_space=pl.ANY)
    vmem = pl.BlockSpec(memory_space=pltpu.VMEM)
    dma = pltpu.SemaphoreType.DMA((MICRO,))
    bf16 = jnp.bfloat16
    return pl.pallas_call(
        functools.partial(cycle_kernel, (shards, head_size, heads)),
        out_shape=jax.ShapeDtypeStruct((MICRO * BLOCK, width // 2), bf16),
        in_specs=[any_space, vmem, any_space, vmem, any_space, any_space],
        out_specs=any_space,
        scratch_shapes=[
            pltpu.VMEM(w_qkv.shape[1:], bf16),
            pltpu.VMEM(w_out.shape[1:], bf16),
            pltpu.VMEM(kv_cache.shape[1:], bf16),
            pltpu.VMEM((MICRO, BLOCK, width), bf16),
            pltpu.VMEM((MICRO, BLOCK, width), bf16),
            pltpu.VMEM((BLOCK, width), bf16),
            pltpu.VMEM((BLOCK, columns), jnp.float32),
            pltpu.VMEM((BLOCK, 128), jnp.float32),
            pltpu.VMEM((MICRO, rows, columns + 256), bf16),
            pltpu.VMEM((MICRO, rows, columns + 256), bf16),
            pltpu.VMEM((MICRO, BLOCK, query_width), bf16),
            pltpu.VMEM((query_width, width // 2), bf16),
            pltpu.VMEM((MICRO // 2, BLOCK, query_width), bf16),
            pltpu.SemaphoreType.DMA((3,)),
            pltpu.SemaphoreType.DMA((1,)),
            pltpu.SemaphoreType.DMA((1,)),
            pltpu.SemaphoreType.DMA((chips - 1,)),
            pltpu.SemaphoreType.DMA((chips - 1,)),
            pltpu.SemaphoreType.DMA((chips,)),
            pltpu.SemaphoreType.DMA((chips,)),
        ]
        + [dma] * 14,
        compiler_params=pltpu.CompilerParams(
            collective_id=0, has_side_effects=True, vmem_limit_bytes=60 << 20
        ),
        name="cycle",
    )(hidden[0], tokens, kv_cache[0], norm_gain, w_qkv[0], w_out[0])


def chosen(batches, devices, *arguments):
    shards = max(2, devices // 4)
    if shards == 2 and devices // shards == 2:
        return cycle_of_two(batches // 2, *arguments)
    return body(*arguments)


def solution(mesh):
    return jax.shard_map(
        functools.partial(chosen, mesh.shape["blk"], mesh.shape["section"]),
        mesh=mesh,
        in_specs=(
            P("section", "blk", None),
            P("blk"),
            P("blk"),
            P("section", "blk", None, None),
            P("section", None),
            P("section", None, None),
            P("section", None, None),
        ),
        out_specs=P("blk", "section"),
        check_vma=False,
    )
```

```python
import functools
import math

import jax
import jax.numpy as jnp
from jax import lax
from jax.experimental import pallas as pl
from jax.experimental.pallas import tpu as pltpu
from jax.sharding import PartitionSpec as P

BLOCK = 64
MICRO = 8


EPSILON = 1e-05
NEGATIVE = -1e30


def partner(value, axis, distance):
    return lax.ppermute(value, axis, [(i, i ^ 1 << distance) for i in range(lax.axis_size(axis))])


def shifted(value, axis, steps):
    count = lax.axis_size(axis)
    pairs = [(source, (source + steps) % count) for source in range(count)]
    return lax.ppermute(value, axis, pairs)


def body(hidden, exit_layer, lengths, kv_cache, norm_gain, w_qkv, w_out):
    devices = lax.axis_size("section")
    index = lax.axis_index("section")
    shards = max(2, devices // 4)
    cycle_size = devices // shards
    segment_bits = cycle_size.bit_length() - 1
    shard_bits = shards.bit_length() - 1
    segment_index = index // shards
    shard_index = index % shards
    own_blocks = hidden[0]
    gain_row = norm_gain[0].astype(jnp.float32)
    proj_weight = w_qkv[0]
    out_weight = w_out[0]
    cache_all = kv_cache[0]
    query_width = out_weight.shape[0]
    head_size = (proj_weight.shape[1] - query_width) // 2
    heads = query_width // head_size
    quarter = proj_weight.shape[0]
    total_width = quarter * shards
    group_rows = BLOCK // shards
    rounds = MICRO // cycle_size
    context = cache_all.shape[1]
    positions = jnp.arange(context, dtype=jnp.int32)
    blank_block = jnp.zeros((BLOCK, quarter), jnp.bfloat16)

    def advance(carry, microstep):
        incoming, arriving, records = carry
        micro_index = microstep - segment_index
        in_range = (micro_index >= 0) & (micro_index < MICRO)
        slot = jnp.clip(micro_index, 0, MICRO - 1)
        on_turn = microstep % cycle_size == 0
        local_slot = jnp.minimum(microstep // cycle_size, rounds - 1)
        own_block = lax.dynamic_slice_in_dim(own_blocks, local_slot * BLOCK, BLOCK, 0)
        exit_rows = lax.dynamic_slice_in_dim(exit_layer, slot * BLOCK, BLOCK)
        own_lengths = lax.dynamic_slice_in_dim(
            lengths, slot * BLOCK + shard_index * group_rows, group_rows
        )
        own_cache = lax.dynamic_slice_in_dim(cache_all, slot * group_rows, group_rows, 0)
        first_input = jnp.where(on_turn, own_block, arriving)
        entering = jnp.where(segment_index == 0, first_input, incoming)
        active = exit_rows > segment_index
        gate = in_range & (jnp.sum(active.astype(jnp.int32)) > 0)

        def local_partials():
            widened = entering.astype(jnp.float32)
            scaled = (widened * gain_row).astype(jnp.bfloat16)
            return (
                jnp.dot(scaled, proj_weight, preferred_element_type=jnp.float32),
                jnp.sum(widened * widened, axis=1),
            )

        def no_partials():
            return (
                jnp.zeros((BLOCK, proj_weight.shape[1]), jnp.float32),
                jnp.zeros((BLOCK,), jnp.float32),
            )

        partial_proj, partial_squares = lax.cond(gate, local_partials, no_partials)
        kept = (partial_proj, partial_squares)
        for level in range(shard_bits):
            bit = shard_bits - 1 - level
            upper = index >> bit & 1
            halves = tuple(
                (piece.reshape((2, piece.shape[0] // 2) + piece.shape[1:]) for piece in kept)
            )
            keep = tuple((jnp.where(upper == 1, half[1], half[0]) for half in halves))
            send = tuple((jnp.where(upper == 1, half[0], half[1]) for half in halves))
            received = partner(send, "section", bit)
            kept = tuple((first + second for first, second in zip(keep, received)))
        own_proj, own_squares = kept

        def local_attention():
            fitted = own_proj * lax.rsqrt(own_squares / total_width + EPSILON)[:, None]
            query = (fitted[:, :query_width] * (1.0 / math.sqrt(head_size))).astype(jnp.bfloat16)
            query = query.reshape(group_rows, heads, head_size)
            key_new = fitted[:, query_width : query_width + head_size].astype(jnp.bfloat16)
            value_new = fitted[:, query_width + head_size :].astype(jnp.bfloat16)
            scores = jnp.einsum(
                "rhd,rcd->rhc",
                query,
                own_cache[:, :, :head_size],
                preferred_element_type=jnp.float32,
            )
            own = jnp.einsum("rhd,rd->rh", query, key_new, preferred_element_type=jnp.float32)
            usable = (positions[None, :] < own_lengths[:, None])[:, None, :]
            scores = jnp.where(usable, scores, NEGATIVE)
            row_top = jnp.maximum(jnp.max(scores, axis=-1), own)
            raw = jnp.where(usable, jnp.exp(scores - row_top[:, :, None]), jnp.float32(0.0))
            raw_own = jnp.exp(own - row_top)
            total = jnp.sum(raw, axis=-1) + raw_own
            weights = (raw / total[:, :, None]).astype(jnp.bfloat16)
            own_weight = (raw_own / total).astype(jnp.bfloat16)
            attended = jnp.einsum(
                "rhc,rcd->rhd",
                weights,
                own_cache[:, :, head_size:],
                preferred_element_type=jnp.float32,
            )
            attended = (
                attended
                + own_weight.astype(jnp.float32)[:, :, None]
                * value_new.astype(jnp.float32)[:, None, :]
            )
            return attended.astype(jnp.bfloat16).reshape(group_rows, query_width)

        def no_attention():
            return jnp.zeros((group_rows, query_width), jnp.bfloat16)

        collected = lax.cond(gate, local_attention, no_attention)
        for level in range(shard_bits):
            bit = level
            other = partner(collected, "section", bit)
            upper = index >> bit & 1
            collected = jnp.where(
                upper == 1,
                jnp.concatenate([other, collected], 0),
                jnp.concatenate([collected, other], 0),
            )

        def local_update():
            branch_out = jnp.dot(collected, out_weight, preferred_element_type=jnp.float32)
            updated = (entering.astype(jnp.float32) + branch_out).astype(jnp.bfloat16)
            return jnp.where(active[:, None], updated, entering)

        def keep_state():
            return entering

        outgoing = lax.cond(gate, local_update, keep_state)
        leaving = in_range & (exit_rows == segment_index + 1)
        previous = lax.dynamic_slice_in_dim(records, slot * BLOCK, BLOCK, 0)
        records = lax.dynamic_update_slice_in_dim(
            records, jnp.where(leaving[:, None], outgoing, previous), slot * BLOCK, 0
        )
        relayed = jnp.where(on_turn & (segment_index > 0), own_block, arriving)
        incoming, arriving = shifted((outgoing, relayed), "section", shards)
        return ((incoming, arriving, records), None)

    start = (blank_block, blank_block, jnp.zeros((MICRO * BLOCK, quarter), jnp.bfloat16))
    carry, _ = lax.scan(advance, start, jnp.arange(MICRO + cycle_size - 1, dtype=jnp.int32))
    kept = carry[2]
    for level in range(segment_bits):
        bit = shard_bits + segment_bits - 1 - level
        upper = index >> bit & 1
        halves = kept.reshape(kept.shape[0], 2, kept.shape[1] // 2)
        keep = jnp.where(upper == 1, halves[:, 1], halves[:, 0])
        send = jnp.where(upper == 1, halves[:, 0], halves[:, 1])
        received = partner(send, "section", bit)
        kept = (keep.astype(jnp.float32) + received.astype(jnp.float32)).astype(jnp.bfloat16)
    return kept


MESH = pl.DeviceIdType.MESH


def cycle_kernel(
    sizes,
    hidden,
    tokens,
    cache_hbm,
    gain,
    wq_hbm,
    wo_hbm,
    out,
    wq,
    wo,
    cache,
    stage,
    ready,
    scaled,
    partial,
    squares,
    psend,
    precv,
    att,
    wx,
    att_in,
    load_sem,
    wy_send,
    wy_recv,
    wz_send,
    wz_recv,
    wd_send,
    wd_recv,
    own_sem,
    h_send,
    h_recv,
    lo_send,
    lo_recv,
    hi_send,
    hi_recv,
    p_send,
    p_recv,
    a_send,
    a_recv,
    r_send,
    r_recv,
    d_send,
    d_recv,
    keep_sem,
):
    shards, head_size, heads = sizes
    index = lax.axis_index("section")
    seg = index // shards
    shard = index % shards
    across = seg * shards + (1 - shard)
    along = (1 - seg) * shards + shard
    corner = (1 - seg) * shards + (1 - shard)
    width = stage.shape[2]
    columns = wq.shape[1]
    query_width = heads * head_size
    half = MICRO // 2
    rows = BLOCK // shards
    span = out.shape[1]
    context = cache.shape[1]
    own_rows = pl.ds(pl.multiple_of(shard * rows, rows), rows)
    other_rows = pl.ds(pl.multiple_of((1 - shard) * rows, rows), rows)

    place_blk = lax.axis_index("blk")
    chips = wz_send.shape[0] + 1
    chip = place_blk // 2
    core = place_blk % 2
    piece = wx.shape[0] // (2 * chips)

    def on_chip(steps):
        return (chip + steps + chips) % chips

    barrier = pltpu.get_barrier_semaphore()
    for peer in (across, along, corner):
        pl.semaphore_signal(barrier, inc=1, device_id={"section": peer}, device_id_type=MESH)
    for steps in range(1, chips):
        pl.semaphore_signal(
            barrier,
            inc=1,
            device_id={"blk": on_chip(steps) * 2 + core},
            device_id_type=MESH,
        )
    pl.semaphore_signal(
        barrier, inc=1, device_id={"blk": chip * 2 + 1 - core}, device_id_type=MESH
    )

    def piece_rows(owner):
        return pl.ds(pl.multiple_of(owner * piece, piece), piece)

    def weight_along():
        return pltpu.make_async_remote_copy(
            src_ref=wo_hbm.at[
                piece_rows(place_blk), pl.ds(pl.multiple_of((1 - seg) * span, 128), span)
            ],
            dst_ref=wx.at[piece_rows(place_blk)],
            send_sem=wy_send.at[0],
            recv_sem=wy_recv.at[0],
            device_id={"section": along},
            device_id_type=MESH,
        )

    def weight_chips(steps, owner):
        return pltpu.make_async_remote_copy(
            src_ref=wx.at[piece_rows(owner)],
            dst_ref=wx.at[piece_rows(owner)],
            send_sem=wz_send.at[steps - 1],
            recv_sem=wz_recv.at[steps - 1],
            device_id={"blk": on_chip(steps) * 2 + core},
            device_id_type=MESH,
        )

    def weight_cores(steps, owner):
        return pltpu.make_async_remote_copy(
            src_ref=wx.at[piece_rows(owner)],
            dst_ref=wx.at[piece_rows(owner)],
            send_sem=wd_send.at[steps],
            recv_sem=wd_recv.at[steps],
            device_id={"blk": chip * 2 + 1 - core},
            device_id_type=MESH,
        )

    def own_copy(i):
        return pltpu.make_async_copy(
            hidden.at[pl.ds(i * BLOCK, BLOCK)], stage.at[i], own_sem.at[i]
        )

    def rest_copy(i):
        return pltpu.make_async_copy(
            hidden.at[pl.ds(i * BLOCK, BLOCK), pl.ds(span, span)],
            stage.at[half + i, :, pl.ds(span, span)],
            own_sem.at[i],
        )

    load_wq = pltpu.make_async_copy(wq_hbm, wq, load_sem.at[0])
    load_cache = pltpu.make_async_copy(cache_hbm, cache, load_sem.at[1])
    load_wo = pltpu.make_async_copy(wo_hbm, wo, load_sem.at[2])

    @pl.when(seg == 0)
    def _():
        own_copy(0).start()

    load_wq.start()
    load_cache.start()

    def place(i):
        return jnp.where(i < half, 2 * i, 2 * (i - half) + 1)

    def hidden_copy(i):
        return pltpu.make_async_remote_copy(
            src_ref=hidden.at[pl.ds(i * BLOCK, BLOCK)],
            dst_ref=stage.at[half + i],
            send_sem=h_send.at[i],
            recv_sem=h_recv.at[i],
            device_id={"section": along},
            device_id_type=MESH,
        )

    def low_copy(i):
        return pltpu.make_async_remote_copy(
            src_ref=ready.at[i, :, pl.ds(0, span)],
            dst_ref=stage.at[i, :, pl.ds(0, span)],
            send_sem=lo_send.at[i],
            recv_sem=lo_recv.at[i],
            device_id={"section": along},
            device_id_type=MESH,
        )

    def high_copy(i):
        return pltpu.make_async_remote_copy(
            src_ref=ready.at[i, :, pl.ds(span, span)],
            dst_ref=stage.at[i, :, pl.ds(span, span)],
            send_sem=hi_send.at[i],
            recv_sem=hi_recv.at[i],
            device_id={"section": along},
            device_id_type=MESH,
        )

    def branch_copy(i, sent_rows):
        return pltpu.make_async_remote_copy(
            src_ref=att.at[i, sent_rows],
            dst_ref=att_in.at[i, sent_rows],
            send_sem=r_send.at[i],
            recv_sem=r_recv.at[i],
            device_id={"section": along},
            device_id_type=MESH,
        )

    def corner_copy(i, sent_rows):
        return pltpu.make_async_remote_copy(
            src_ref=att.at[i, sent_rows],
            dst_ref=att_in.at[i, sent_rows],
            send_sem=d_send.at[i],
            recv_sem=d_recv.at[i],
            device_id={"section": corner},
            device_id_type=MESH,
        )

    def partial_copy(i):
        return pltpu.make_async_remote_copy(
            src_ref=psend.at[i],
            dst_ref=precv.at[i],
            send_sem=p_send.at[i],
            recv_sem=p_recv.at[i],
            device_id={"section": across},
            device_id_type=MESH,
        )

    def attended_copy(i, sent_rows):
        return pltpu.make_async_remote_copy(
            src_ref=att.at[i, sent_rows],
            dst_ref=att.at[i, sent_rows],
            send_sem=a_send.at[i],
            recv_sem=a_recv.at[i],
            device_id={"section": across},
            device_id_type=MESH,
        )

    def out_rows(i):
        return pl.ds(pl.multiple_of(place(i) * BLOCK, BLOCK), BLOCK)

    def kept_copy(i):
        return pltpu.make_async_copy(
            ready.at[i, :, pl.ds(span, span)], out.at[out_rows(i)], keep_sem.at[i]
        )

    def final_copy(i):
        return pltpu.make_async_copy(
            stage.at[i, :, pl.ds(0, span)], out.at[out_rows(i)], keep_sem.at[i]
        )

    def spread():
        weight_along().wait_recv()
        for steps in range(1, chips):
            weight_chips(steps, place_blk).start()
        weight_cores(0, place_blk).start()

    def pass_on():
        for steps in range(1, chips):
            owner = on_chip(-steps) * 2 + core
            weight_chips(steps, owner).wait_recv()
            weight_cores(steps, owner).start()

    def gathered():
        for steps in range(chips):
            weight_cores(steps, on_chip(-steps) * 2 + 1 - core).wait_recv()

    pl.semaphore_wait(barrier, chips + 3)

    @pl.when(seg == 0)
    def _():
        weight_along().start()
        for i in range(1, half):
            own_copy(i).start()

    @pl.when(seg == 1)
    def _():
        hidden_copy(0).start()
        weight_along().start()
        for i in range(1, half):
            hidden_copy(i).start()
        for i in range(half):
            rest_copy(i).start()
        spread()

    def project(i):
        local = (seg == 0) & (i < half)

        @pl.when(local)
        def _():
            own_copy(i).wait()

        @pl.when((seg == 0) & (i == half))
        def _():
            spread()

        @pl.when((seg == 0) & (i >= half))
        def _():
            hidden_copy(i - half).wait_recv()

        @pl.when((seg == 1) & (i == half - 1))
        def _():
            pass_on()

        @pl.when((seg == 1) & (i < half))
        def _():
            high_copy(i).wait_recv()

        @pl.when((seg == 1) & (i == half))
        def _():
            gathered()

        @pl.when((seg == 1) & (i >= half))
        def _():
            rest_copy(i - half).wait()
            branch_copy(i, own_rows).wait_recv()
            corner_copy(i, other_rows).wait_recv()
            depth = tokens[pl.ds(pl.multiple_of(place(i) * BLOCK, BLOCK), BLOCK), :][:, 0:1]
            size = min(span, 512)
            for start in range(0, span, size):
                branch = jnp.dot(
                    att_in[i],
                    wx[:, pl.ds(start, size)],
                    preferred_element_type=jnp.float32,
                )
                cols = pl.ds(span + start, size)
                before = stage[i, :, cols].astype(jnp.float32)
                stage[i, :, cols] = jnp.where(depth > 0, before + branch, before).astype(
                    jnp.bfloat16
                )

        @pl.when(seg == 1)
        def _():
            low_copy(i).wait_recv()

        @pl.when(i == 0)
        def _():
            load_wq.wait()
            load_wo.start()

        chunk = min(width, 512)
        total = jnp.zeros((BLOCK, 1), jnp.float32)
        for start in range(0, width, chunk):
            cols = pl.ds(start, chunk)
            piece = stage[i, :, cols].astype(jnp.float32)
            total = total + jnp.sum(piece * piece, axis=1, keepdims=True)
            scaled[:, cols] = (piece * gain[:, cols].astype(jnp.float32)).astype(jnp.bfloat16)
        squares[...] = jnp.broadcast_to(total, squares.shape)
        step = 512
        for start in range(0, columns, step):
            cols = pl.ds(start, min(step, columns - start))
            partial[:, cols] = jnp.dot(
                scaled[...], wq[:, cols], preferred_element_type=jnp.float32
            )
        psend[i, :, pl.ds(0, columns)] = partial[other_rows, :].astype(jnp.bfloat16)
        theirs = squares[other_rows, :]
        coarse = theirs.astype(jnp.bfloat16)
        fine = (theirs - coarse.astype(jnp.float32)).astype(jnp.bfloat16)
        psend[i, :, pl.ds(columns, 128)] = coarse
        psend[i, :, pl.ds(columns + 128, 128)] = fine
        partial_copy(i).start()

    def attend_rows(i):
        @pl.when(i == 0)
        def _():
            load_cache.wait()

        partial_copy(i).wait_recv()
        coarse = precv[i, :, pl.ds(columns, 128)].astype(jnp.float32)
        fine = precv[i, :, pl.ds(columns + 128, 128)].astype(jnp.float32)
        total_squares = squares[own_rows, :] + coarse + fine
        factor = lax.rsqrt(total_squares / (width * shards) + EPSILON)[:, :1]
        fitted = (
            partial[own_rows, :] + precv[i, :, pl.ds(0, columns)].astype(jnp.float32)
        ) * factor
        scale = 1.0 / math.sqrt(head_size)
        query = jnp.concatenate(
            [fitted[:, h * head_size : (h + 1) * head_size] for h in range(heads)], axis=0
        )
        query = (query * scale).astype(jnp.bfloat16)
        key_new = fitted[:, query_width : query_width + head_size].astype(jnp.bfloat16)
        value_new = fitted[:, query_width + head_size :].astype(jnp.bfloat16)
        key_new = jnp.concatenate([key_new.astype(jnp.float32)] * heads, axis=0)
        value_new = jnp.concatenate([value_new.astype(jnp.float32)] * heads, axis=0)
        start = pl.multiple_of(place(i) * rows, rows)
        held = cache[pl.ds(start, rows)].reshape(rows * context, 2 * head_size)
        scores = lax.dot_general(
            query,
            held[:, :head_size],
            (((1,), (1,)), ((), ())),
            preferred_element_type=jnp.float32,
        )
        own = jnp.sum(query.astype(jnp.float32) * key_new, axis=1, keepdims=True)
        limits = tokens[pl.ds(pl.multiple_of(place(i) * BLOCK + shard * rows, rows), rows), :][:, 1:2]
        row = lax.broadcasted_iota(jnp.int32, (rows, 1), 0) * context
        low = jnp.concatenate([row] * heads, axis=0)
        high = jnp.concatenate([row + limits] * heads, axis=0)
        column = lax.broadcasted_iota(jnp.int32, scores.shape, 1)
        usable = (column >= low) & (column < high)
        scores = jnp.where(usable, scores, NEGATIVE)
        row_top = jnp.maximum(jnp.max(scores, axis=1, keepdims=True), own)
        raw = jnp.where(usable, jnp.exp(scores - row_top), 0.0)
        raw_own = jnp.exp(own - row_top)
        total = jnp.sum(raw, axis=1, keepdims=True) + raw_own
        weights = (raw / total).astype(jnp.bfloat16)
        own_weight = (raw_own / total).astype(jnp.bfloat16).astype(jnp.float32)
        attended = jnp.dot(
            weights, held[:, head_size:], preferred_element_type=jnp.float32
        )
        attended = (attended + own_weight * value_new).astype(jnp.bfloat16)
        att[i, own_rows, :] = jnp.concatenate(
            [attended[h * rows : (h + 1) * rows] for h in range(heads)], axis=1
        )
        attended_copy(i, own_rows).start()

        @pl.when((seg == 1) | (i >= half))
        def _():
            corner_copy(i, own_rows).start()
            branch_copy(i, own_rows).start()

    def update(i):
        @pl.when(i == 0)
        def _():
            load_wo.wait()

        attended_copy(i, other_rows).wait_recv()
        depth = tokens[pl.ds(pl.multiple_of(place(i) * BLOCK, BLOCK), BLOCK), :][:, 0:1]
        active = depth > seg
        step = min(span, 512)

        def fill(first):
            for start in range(first, first + span, step):
                cols = pl.ds(start, step)
                branch = jnp.dot(att[i], wo[:, cols], preferred_element_type=jnp.float32)
                before = stage[i, :, cols].astype(jnp.float32)
                ready[i, :, cols] = jnp.where(active, before + branch, before).astype(jnp.bfloat16)

        @pl.when(seg == 0)
        def _():
            fill(0)
            low_copy(i).start()

        @pl.when((seg == 1) | (i < half))
        def _():
            fill(span)

        @pl.when((seg == 0) & (i < half))
        def _():
            high_copy(i).start()

        @pl.when(seg == 1)
        def _():
            kept_copy(i).start()

    def step(i, carry):
        @pl.when(i < MICRO)
        def _():
            project(i)

        @pl.when(i > 0)
        def _():
            update(i - 1)

        @pl.when(i < MICRO)
        def _():
            attend_rows(i)

        return carry

    lax.fori_loop(0, MICRO + 1, step, 0)

    def finish(i, carry):
        branch_copy(i, own_rows).wait_recv()
        corner_copy(i, other_rows).wait_recv()
        depth = tokens[pl.ds(pl.multiple_of(place(i) * BLOCK, BLOCK), BLOCK), :][:, 0:1]
        size = min(span, 512)
        for start in range(0, span, size):
            cols = pl.ds(start, size)
            branch = jnp.dot(att_in[i], wx[:, cols], preferred_element_type=jnp.float32)
            before = ready[i, :, cols].astype(jnp.float32)
            stage[i, :, cols] = jnp.where(depth > 1, before + branch, before).astype(jnp.bfloat16)
        final_copy(i).start()
        return carry

    @pl.when(seg == 0)
    def _():
        pass_on()
        gathered()
        lax.fori_loop(0, MICRO, finish, 0)

    def drain(i, carry):
        partial_copy(i).wait_send()
        attended_copy(i, own_rows).wait_send()

        @pl.when(seg == 0)
        def _():
            low_copy(i).wait_send()
            final_copy(i).wait()

        @pl.when(seg == 1)
        def _():
            kept_copy(i).wait()

        @pl.when((seg == 1) | (i >= half))
        def _():
            branch_copy(i, own_rows).wait_send()
            corner_copy(i, own_rows).wait_send()

        return carry

    lax.fori_loop(0, MICRO, drain, 0)

    weight_along().wait_send()
    for steps in range(1, chips):
        weight_chips(steps, place_blk).wait_send()
    for steps in range(chips):
        weight_cores(steps, on_chip(-steps) * 2 + core).wait_send()

    @pl.when(seg == 0)
    def _():
        for i in range(half):
            high_copy(i).wait_send()

    @pl.when(seg == 1)
    def _():
        for i in range(half):
            hidden_copy(i).wait_send()


def cycle_of_two(chips, hidden, exit_layer, lengths, kv_cache, norm_gain, w_qkv, w_out):
    shards = 2
    width = w_qkv.shape[1]
    columns = w_qkv.shape[2]
    query_width = w_out.shape[1]
    head_size = (columns - query_width) // 2
    heads = query_width // head_size
    rows = BLOCK // shards
    tokens = jnp.stack([exit_layer, lengths], axis=1)
    any_space = pl.BlockSpec(memory_space=pl.ANY)
    vmem = pl.BlockSpec(memory_space=pltpu.VMEM)
    dma = pltpu.SemaphoreType.DMA((MICRO,))
    bf16 = jnp.bfloat16
    return pl.pallas_call(
        functools.partial(cycle_kernel, (shards, head_size, heads)),
        out_shape=jax.ShapeDtypeStruct((MICRO * BLOCK, width // 2), bf16),
        in_specs=[any_space, vmem, any_space, vmem, any_space, any_space],
        out_specs=any_space,
        scratch_shapes=[
            pltpu.VMEM(w_qkv.shape[1:], bf16),
            pltpu.VMEM(w_out.shape[1:], bf16),
            pltpu.VMEM(kv_cache.shape[1:], bf16),
            pltpu.VMEM((MICRO, BLOCK, width), bf16),
            pltpu.VMEM((MICRO, BLOCK, width), bf16),
            pltpu.VMEM((BLOCK, width), bf16),
            pltpu.VMEM((BLOCK, columns), jnp.float32),
            pltpu.VMEM((BLOCK, 128), jnp.float32),
            pltpu.VMEM((MICRO, rows, columns + 256), bf16),
            pltpu.VMEM((MICRO, rows, columns + 256), bf16),
            pltpu.VMEM((MICRO, BLOCK, query_width), bf16),
            pltpu.VMEM((query_width, width // 2), bf16),
            pltpu.VMEM((MICRO, BLOCK, query_width), bf16),
            pltpu.SemaphoreType.DMA((3,)),
            pltpu.SemaphoreType.DMA((1,)),
            pltpu.SemaphoreType.DMA((1,)),
            pltpu.SemaphoreType.DMA((chips - 1,)),
            pltpu.SemaphoreType.DMA((chips - 1,)),
            pltpu.SemaphoreType.DMA((chips,)),
            pltpu.SemaphoreType.DMA((chips,)),
        ]
        + [dma] * 16,
        compiler_params=pltpu.CompilerParams(
            collective_id=0, has_side_effects=True, vmem_limit_bytes=60 << 20
        ),
        name="cycle",
    )(hidden[0], tokens, kv_cache[0], norm_gain, w_qkv[0], w_out[0])


def chosen(batches, devices, *arguments):
    shards = max(2, devices // 4)
    if shards == 2 and devices // shards == 2:
        return cycle_of_two(batches // 2, *arguments)
    return body(*arguments)


def solution(mesh):
    return jax.shard_map(
        functools.partial(chosen, mesh.shape["blk"], mesh.shape["section"]),
        mesh=mesh,
        in_specs=(
            P("section", "blk", None),
            P("blk"),
            P("blk"),
            P("section", "blk", None, None),
            P("section", None),
            P("section", None, None),
            P("section", None, None),
        ),
        out_specs=P("blk", "section"),
        check_vma=False,
    )
```
